32 devices in a mesh: dp: 2 (over y), seq: 16 (over z, x, core).
Axes of the slice: x: 2, y: 2, z: 4, core: 2. Of those that a mesh axis runs over, the one named last changes fastest.
Arguments:
- features: bfloat16 [4096, 320], P(('dp', 'seq')), parts along dimension 0, may hold values from -40 to 40
- hint: bfloat16 [4096, 320], P(('dp', 'seq')), parts along dimension 0, may hold values from -6 to 6
- conv_weight: bfloat16 [3, 3, 320, 320], replicated, may hold values from -0.109375 to 0.109375
- conv_bias: float32 [320], replicated, may hold values from -3 to 3
- zero_weight: bfloat16 [320, 320], replicated, may hold values from -0.3125 to 0.3125
- zero_bias: float32 [320], replicated, may hold values from -2 to 2
- group_gain: float32 [320], replicated, may hold values from 0.5 to 1.5
- proj_in: bfloat16 [320, 320], replicated, may hold values from -0.3125 to 0.3125
- norm_gain: float32 [320], replicated, may hold values from 0.5 to 1.5
- query_weight: bfloat16 [320, 320], replicated, may hold values from -2 to 2
- key_weight: bfloat16 [320, 320], replicated, may hold values from -2 to 2
- value_weight: bfloat16 [320, 320], replicated, may hold values from -0.3125 to 0.3125
- attn_out: bfloat16 [320, 320], replicated, may hold values from -0.3125 to 0.3125
- proj_out: bfloat16 [320, 320], replicated, may hold values from -0.3125 to 0.3125
Outputs:
- block_out: bfloat16 [4096, 320], P(('dp', 'seq')), parts along dimension 0
The draws below stay inside these ranges and needn't reach their ends.
There are 2 independent parts, one for each index of `dp`. The reference program is written for one: setup_inputs(seed, part) draws one part's arguments, and reference() takes and returns one part's arrays. A program takes and returns all parts, laid end to end along the dimension named above; an argument that names none is the same for every part. Nothing has to cross between parts.
All inputs are finite; a program needn't handle non-finite values.
Results may differ from the reference program's by a relative error of at most 0.023.
Values may be sent and summed in bfloat16 or wider, within the bound.
A program may use at most 64 MiB of HBM per device.

```python
import math
import jax
import jax.numpy as jnp
from jax import lax

C = 320
HEADS = 8
GROUPS = 32
WIDTH = 128
SEQ = 2048


def draw_features(key, part):
    sub_keys = [jax.random.fold_in(key, 11 + index) for index in range(8)]
    position = jnp.arange(SEQ, dtype=jnp.float32) / (SEQ - 1)
    noise_vals = jnp.clip(jax.random.normal(sub_keys[0], (SEQ, C), jnp.float32), -4.0, 4.0)
    rise_row = 1.0 + 2.0 * position
    row_scale = jnp.exp(jax.random.uniform(sub_keys[1], (SEQ,), jnp.float32, math.log(0.3), 0.0))
    col_scale = jnp.exp(jax.random.uniform(sub_keys[2], (C,), jnp.float32, math.log(0.5), math.log(2.0)))
    group_off = jax.random.normal(sub_keys[4], (GROUPS,), jnp.float32)
    offset_col = jnp.repeat(group_off, C // GROUPS) + 0.3 * jax.random.normal(sub_keys[3], (C,), jnp.float32)
    offset_rise = 0.3 + 2.7 * position
    drawn = offset_rise[:, None] * offset_col[None, :] + (rise_row * row_scale)[:, None] * col_scale[None, :] * noise_vals
    return jnp.clip(drawn, -40.0, 40.0).astype(jnp.bfloat16)


def draw_hint(key, part):
    sub_keys = [jax.random.fold_in(key, 41 + index) for index in range(6)]
    position = jnp.arange(SEQ, dtype=jnp.float32) / (SEQ - 1)
    sign_col = jnp.where(jax.random.bernoulli(sub_keys[0], 0.5, (C,)), 1.0, -1.0)
    ramp_size = jax.random.uniform(sub_keys[1], (C,), jnp.float32, 0.5, 1.5)
    offset_col = 1.5 * jax.random.normal(sub_keys[2], (C,), jnp.float32)
    noise_vals = jnp.clip(jax.random.normal(sub_keys[3], (SEQ, C), jnp.float32), -4.0, 4.0)
    ramp_amp = 2.5
    ramp = ramp_amp * (2.0 * position - 1.0)
    drawn = offset_col[None, :] + ramp[:, None] * (sign_col * ramp_size)[None, :] + noise_vals
    return jnp.clip(drawn, -6.0, 6.0).astype(jnp.bfloat16)


def weight_pair(key):
    base_key = jax.random.fold_in(key, 71)
    first_mat = jax.random.normal(jax.random.fold_in(base_key, 1), (C, C), jnp.float32)
    second_mat = jax.random.normal(jax.random.fold_in(base_key, 2), (C, C), jnp.float32)
    query_mat = first_mat * (1.5 / math.sqrt(C))
    key_mat = -(first_mat + 0.3 * second_mat) * (1.5 / math.sqrt(C))
    return (jnp.clip(query_mat, -2.0, 2.0), jnp.clip(key_mat, -2.0, 2.0))


def draw_query_weight(key, part):
    return weight_pair(key)[0].astype(jnp.bfloat16)


def draw_key_weight(key, part):
    return weight_pair(key)[1].astype(jnp.bfloat16)


def bell_draw(key, dims, scale, limit, kind=jnp.bfloat16):
    array = scale * jax.random.normal(key, dims, jnp.float32)
    return jnp.clip(array, min=-limit, max=limit).astype(kind)


def setup_inputs(seed: int = 0, part: int = 0) -> dict:
    keys = jax.random.split(jax.random.key(seed), 15)
    own_keys = jax.random.split(jax.random.fold_in(keys[14], part), 15)
    return {
        "features": draw_features(jax.random.fold_in(jax.random.fold_in(keys[14], part), 71), part),
        "hint": draw_hint(jax.random.fold_in(jax.random.fold_in(keys[14], part), 71), part),
        "conv_weight": bell_draw(keys[2], (3, 3, C, C), (9 * C) ** -0.5, 0.109375),
        "conv_bias": bell_draw(keys[3], (C,), 0.5, 3.0, jnp.float32),
        "zero_weight": bell_draw(keys[4], (C, C), C ** -0.5, 0.3125),
        "zero_bias": bell_draw(keys[5], (C,), 0.3, 2.0, jnp.float32),
        "group_gain": jnp.clip(1.0 + 0.1 * jax.random.normal(keys[6], (C,), jnp.float32), 0.5, 1.5),
        "proj_in": bell_draw(keys[7], (C, C), C ** -0.5, 0.3125),
        "norm_gain": jnp.clip(1.0 + 0.1 * jax.random.normal(keys[8], (C,), jnp.float32), 0.5, 1.5),
        "query_weight": draw_query_weight(jax.random.fold_in(keys[14], 71), part),
        "key_weight": draw_key_weight(jax.random.fold_in(keys[14], 71), part),
        "value_weight": bell_draw(keys[11], (C, C), C ** -0.5, 0.3125),
        "attn_out": bell_draw(keys[12], (C, C), C ** -0.5, 0.3125),
        "proj_out": bell_draw(keys[13], (C, C), C ** -0.5, 0.3125),
    }


norm_eps = 1e-06
layer_eps = 1e-05

def conv_extended(extended, conv_weight, conv_bias, width):
    line_count = extended.shape[0] // width - 2
    channels = extended.shape[1]
    lattice = extended.reshape(line_count + 2, width, channels)
    padded = jnp.pad(lattice, ((0, 0), (1, 1), (0, 0)))
    summed = jnp.zeros((line_count * width, conv_weight.shape[3]), jnp.float32)
    for row_shift in range(3):
        for col_shift in range(3):
            window = padded[row_shift:row_shift + line_count, col_shift:col_shift + width]
            window = window.reshape(line_count * width, channels)
            summed = summed + jnp.dot(window, conv_weight[row_shift, col_shift], preferred_element_type=jnp.float32)
    return summed + conv_bias

def control_merge(features, extended, conv_weight, conv_bias, zero_weight, zero_bias):
    control = jax.nn.silu(conv_extended(extended, conv_weight, conv_bias, WIDTH)).astype(jnp.bfloat16)
    branch = jnp.dot(control, zero_weight, preferred_element_type=jnp.float32) + zero_bias
    return (features.astype(jnp.float32) + branch).astype(jnp.bfloat16)

def group_apply(merged, mean_group, var_group, group_gain):
    per_group = merged.shape[1] // mean_group.shape[0]
    mean_chan = jnp.repeat(mean_group, per_group)
    inv_chan = jnp.repeat(lax.rsqrt(var_group + norm_eps), per_group)
    return ((merged.astype(jnp.float32) - mean_chan) * inv_chan * group_gain).astype(jnp.bfloat16)

def project_norm(grouped, proj_in, norm_gain):
    inner_rows = jnp.dot(grouped, proj_in, preferred_element_type=jnp.float32).astype(jnp.bfloat16)
    widened = inner_rows.astype(jnp.float32)
    centre = lax.optimization_barrier(jnp.mean(widened, axis=1, keepdims=True))
    spread = lax.optimization_barrier(jnp.mean(jnp.square(widened - centre), axis=1, keepdims=True))
    normed = ((widened - centre) * lax.rsqrt(spread + layer_eps) * norm_gain).astype(jnp.bfloat16)
    return (inner_rows, normed)

def reference(features, hint, conv_weight, conv_bias, zero_weight, zero_bias, group_gain, proj_in, norm_gain, query_weight, key_weight, value_weight, attn_out, proj_out):
    seq_len, channels = features.shape
    extended = jnp.pad(hint, ((WIDTH, WIDTH), (0, 0)))
    merged = control_merge(features, extended, conv_weight, conv_bias, zero_weight, zero_bias)
    widened = merged.astype(jnp.float32)
    per_group = channels // GROUPS
    entry_count = seq_len * per_group
    mean_group = lax.optimization_barrier(jnp.sum(widened.reshape(seq_len, GROUPS, per_group), axis=(0, 2))) / entry_count
    centred = widened - jnp.repeat(mean_group, per_group)
    var_group = lax.optimization_barrier(jnp.sum(jnp.square(centred).reshape(seq_len, GROUPS, per_group), axis=(0, 2))) / entry_count
    grouped = group_apply(merged, mean_group, var_group, group_gain)
    inner_rows, normed = project_norm(grouped, proj_in, norm_gain)
    head_dim = channels // HEADS

    def project(weight):
        made = jnp.dot(normed, weight, preferred_element_type=jnp.float32).astype(jnp.bfloat16)
        return made.reshape(seq_len, HEADS, head_dim)
    queries = project(query_weight)
    keys_wide = project(key_weight).astype(jnp.float32)
    values_wide = project(value_weight).astype(jnp.float32)
    block_len = math.gcd(seq_len, 512)
    score_scale = 1.0 / math.sqrt(head_dim)

    def attend(query_block):
        scores = jnp.einsum('qhd,khd->hqk', query_block.astype(jnp.float32), keys_wide) * score_scale
        row_max = lax.optimization_barrier(jnp.max(scores, axis=2, keepdims=True))
        weights = jnp.exp(scores - row_max)
        running_sum = lax.optimization_barrier(jnp.sum(weights, axis=2))
        rounded = lax.optimization_barrier(weights.astype(jnp.bfloat16)).astype(jnp.float32)
        weighted = jnp.einsum('hqk,khd->qhd', rounded, values_wide)
        return weighted / jnp.transpose(running_sum)[:, :, None]
    blocks = queries.reshape(seq_len // block_len, block_len, HEADS, head_dim)
    attended = lax.map(attend, blocks).reshape(seq_len, channels).astype(jnp.bfloat16)
    after_attn = (inner_rows.astype(jnp.float32) + jnp.dot(attended, attn_out, preferred_element_type=jnp.float32)).astype(jnp.bfloat16)
    return (merged.astype(jnp.float32) + jnp.dot(after_attn, proj_out, preferred_element_type=jnp.float32)).astype(jnp.bfloat16)
```

```python
import functools
import math

import jax
import jax.numpy as jnp
from jax import lax
from jax.experimental import pallas as pl
from jax.experimental.pallas import tpu as pltpu
from jax.sharding import PartitionSpec as P

HEADS = 8
GROUPS = 32
WIDTH = 128
CORES = 2

norm_eps = 1e-06
layer_eps = 1e-05
MESH = pl.DeviceIdType.MESH
F32 = jnp.float32
BF16 = jnp.bfloat16


def mm(x, y):
    return jnp.dot(x, y, preferred_element_type=F32)


def block_kernel(
    n, rows_a, rows_b,
    features, hint, conv_bias, zero_bias, group_gain, norm_gain,
    conv_hbm, zero_hbm, proj_in_hbm, query_hbm, key_hbm, value_hbm, attn_hbm, proj_hbm,
    out,
    conv_w, zero_w, proj_in_w, query_w, key_w, value_w, attn_w, proj_w,
    ext, gathered, normed_all, qmask, scores, mixed,
    load_sem, halo_send, halo_recv, send_sem, recv_sem,
):
    tokens, channels = features.shape
    head_dim = channels // HEADS
    per_group = channels // GROUPS
    me = lax.axis_index("seq")
    core = lax.rem(me, CORES)
    chip = lax.div(me, CORES)
    b = lax.rem(chip, rows_b)
    a = lax.div(chip, rows_b)

    def device(aa, bb, cc):
        return (aa * rows_b + bb) * CORES + cc

    loads = {}
    for slot, (name, src, dst) in enumerate((
        ("conv", conv_hbm, conv_w), ("zero", zero_hbm, zero_w), ("proj_in", proj_in_hbm, proj_in_w),
        ("query", query_hbm, query_w), ("key", key_hbm, key_w), ("value", value_hbm, value_w),
        ("attn", attn_hbm, attn_w), ("proj", proj_hbm, proj_w),
    )):
        loads[name] = pltpu.make_async_copy(src, dst, load_sem.at[slot])
        loads[name].start()

    barrier = pltpu.get_barrier_semaphore()
    always = jnp.int32(1)
    peers = [
        (me > 0, me - 1), (me < n - 1, me + 1),
        (a > 0, device(a - 1, b, core)), (a < rows_a - 1, device(a + 1, b, core)),
        (None, device(a, b, 1 - core)),
    ]
    for k in range(1, rows_b):
        peers.append((None, device(a, lax.rem(b + k, rows_b), core)))
    count = jnp.int32(0)
    for cond, peer in peers:
        def greet(peer=peer):
            pl.semaphore_signal(barrier, inc=1, device_id={"seq": peer}, device_id_type=MESH)
        if cond is None:
            greet()
            count = count + always
        else:
            pl.when(cond)(greet)
            count = count + cond.astype(jnp.int32)
    pl.semaphore_wait(barrier, count)

    to_next = pltpu.make_async_remote_copy(
        hint.at[pl.ds(tokens - WIDTH, WIDTH)], ext.at[pl.ds(0, WIDTH)],
        halo_send.at[0], halo_recv.at[0], device_id={"seq": me + 1}, device_id_type=MESH)
    to_prev = pltpu.make_async_remote_copy(
        hint.at[pl.ds(0, WIDTH)], ext.at[pl.ds(WIDTH + tokens, WIDTH)],
        halo_send.at[1], halo_recv.at[1], device_id={"seq": me - 1}, device_id_type=MESH)
    pl.when(me < n - 1)(to_next.start)
    pl.when(me > 0)(to_prev.start)

    ext[pl.ds(WIDTH, tokens)] = hint[...]

    @pl.when(me == 0)
    def _():
        ext[pl.ds(0, WIDTH)] = jnp.zeros((WIDTH, channels), BF16)

    @pl.when(me == n - 1)
    def _():
        ext[pl.ds(WIDTH + tokens, WIDTH)] = jnp.zeros((WIDTH, channels), BF16)

    loads["conv"].wait()
    middle = hint[...]
    taps = [mm(middle, conv_w[1, d]) for d in range(3)]
    pl.when(me > 0)(to_next.wait_recv)
    pl.when(me < n - 1)(to_prev.wait_recv)
    for dy in (0, 2):
        lines = ext[pl.ds(dy * WIDTH, tokens)]
        taps = [taps[d] + mm(lines, conv_w[dy, d]) for d in range(3)]
    column = lax.rem(lax.broadcasted_iota(jnp.int32, (tokens, channels), 0), WIDTH)
    left = jnp.where(column == 0, 0.0, pltpu.roll(taps[0], 1, 0))
    right = jnp.where(column == WIDTH - 1, 0.0, pltpu.roll(taps[2], tokens - 1, 0))
    conv = left + taps[1] + right + conv_bias[...]
    control = (conv / (1.0 + jnp.exp(-conv))).astype(BF16)
    loads["zero"].wait()
    merged = (features[...].astype(F32) + (mm(control, zero_w[...]) + zero_bias[...])).astype(BF16)
    gathered[me] = merged

    pending = []

    def send(src, target, cond):
        slot = len(pending)
        copy = pltpu.make_async_remote_copy(
            gathered.at[src], gathered.at[src], send_sem.at[slot], recv_sem.at[src],
            device_id={"seq": target}, device_id_type=MESH)
        pending.append((cond, copy))
        if cond is None:
            copy.start()
        else:
            pl.when(cond)(copy.start)

    def arrive(src, cond):
        def wait():
            pltpu.make_async_remote_copy(
                gathered.at[src], gathered.at[src], send_sem.at[0], recv_sem.at[src],
                device_id={"seq": me}, device_id_type=MESH).wait_recv()
        if cond is None:
            wait()
        else:
            pl.when(cond)(wait)

    def spread(src, cond):
        for k in range(1, rows_b):
            send(src, device(a, lax.rem(b + k, rows_b), core), cond)
        send(src, device(a, b, 1 - core), cond)

    def cross(step):
        for k in range(1, rows_b):
            bb = lax.rem(b + k, rows_b)
            for sign in ((1,) if step == 0 else (-1, 1)):
                aa = a + sign * step
                cond = None if step == 0 else ((aa >= 0) & (aa < rows_a))
                src = device(aa, bb, core)
                arrive(src, cond)
                send(src, device(a, b, 1 - core), cond)

    send(me, device(a + 1, b, core), a < rows_a - 1)
    send(me, device(a - 1, b, core), a > 0)
    spread(me, None)
    for step in range(1, rows_a):
        low, high = device(a - step, b, core), device(a + step, b, core)
        has_low, has_high = a - step >= 0, a + step < rows_a
        arrive(low, has_low)
        send(low, device(a + 1, b, core), has_low & (a < rows_a - 1))
        spread(low, has_low)
        arrive(high, has_high)
        send(high, device(a - 1, b, core), has_high & (a > 0))
        spread(high, has_high)
        cross(step - 1)
    cross(rows_a - 1)
    for k in range(rows_a * rows_b):
        arrive(k * CORES + 1 - core, None)

    entry_count = tokens * n * per_group
    row_group = lax.div(lax.broadcasted_iota(jnp.int32, (channels, channels), 0), jnp.int32(per_group))
    col_group = lax.div(lax.broadcasted_iota(jnp.int32, (channels, channels), 1), jnp.int32(per_group))
    same = (row_group == col_group).astype(F32)

    def group_mean(partial):
        total = jnp.dot(partial, same, preferred_element_type=F32, precision=lax.Precision.HIGHEST)
        return jnp.sum(total, axis=0, keepdims=True) / entry_count

    def fold_rows(x):
        return jnp.sum(x.reshape(tokens // 8, 8, channels), axis=0)

    def add_sum(k, acc):
        return acc + fold_rows(gathered[k].astype(F32))

    zero_acc = jnp.zeros((8, channels), F32)
    mean = group_mean(lax.fori_loop(0, n, add_sum, zero_acc))

    def add_square(k, acc):
        return acc + fold_rows(jnp.square(gathered[k].astype(F32) - mean))

    var = group_mean(lax.fori_loop(0, n, add_square, zero_acc))
    inv = lax.rsqrt(var + norm_eps)
    gain = group_gain[...]
    loads["proj_in"].wait()

    def project_norm(block):
        grouped = ((block.astype(F32) - mean) * inv * gain).astype(BF16)
        inner = mm(grouped, proj_in_w[...]).astype(BF16)
        wide = inner.astype(F32)
        centred = wide - jnp.mean(wide, axis=1, keepdims=True)
        spread_row = jnp.mean(jnp.square(centred), axis=1, keepdims=True)
        return wide, (centred * lax.rsqrt(spread_row + layer_eps) * norm_gain[...]).astype(BF16)

    inner_own, normed_own = project_norm(merged)
    chunk = 4 if n % 4 == 0 else 1

    def norm_chunk(k, carry):
        block = gathered[pl.ds(k * chunk, chunk)].reshape(chunk * tokens, channels)
        normed_all[pl.ds(pl.multiple_of(k * chunk * tokens, chunk * tokens), chunk * tokens)] = project_norm(block)[1]
        return carry

    lax.fori_loop(0, n // chunk, norm_chunk, 0)

    loads["query"].wait()
    loads["key"].wait()
    queries = mm(normed_own, query_w[...])
    queries_t = jnp.transpose(queries)
    row_head = lax.div(lax.broadcasted_iota(jnp.int32, (channels, tokens), 0), jnp.int32(head_dim))
    for h in range(HEADS):
        qmask[:, h * tokens:(h + 1) * tokens] = jnp.where(row_head == h, queries_t, 0.0).astype(BF16)
    scale = math.log2(math.e) / math.sqrt(head_dim)
    qmask[...] = (mm(key_w[...], qmask[...]) * scale).astype(BF16)

    loads["value"].wait()
    value_t = jnp.transpose(value_w[...].astype(F32)).astype(BF16)
    pair = 2 * tokens
    keys = normed_all[...]
    for h2 in range(HEADS // 2):
        cols = slice(h2 * pair, (h2 + 1) * pair)
        scores[...] = mm(keys, qmask[:, cols])
        top = jnp.max(scores[...], axis=0, keepdims=True)
        weights = jnp.exp2(scores[...] - top)
        total = jnp.sum(weights, axis=0, keepdims=True)
        folded = lax.dot_general(keys, weights.astype(BF16), (((0,), (0,)), ((), ())),
                                 preferred_element_type=F32)
        folded = (folded / total).astype(BF16)
        values = mm(value_t, folded)
        for j in range(2):
            h = 2 * h2 + j
            mixed[pl.ds(h * head_dim, head_dim)] = values[h * head_dim:(h + 1) * head_dim, j * tokens:(j + 1) * tokens]
    attended = jnp.transpose(mixed[...]).astype(BF16)
    loads["attn"].wait()
    loads["proj"].wait()
    after = (inner_own + mm(attended, attn_w[...])).astype(BF16)
    out[...] = (merged.astype(F32) + mm(after, proj_w[...])).astype(BF16)

    pl.when(me < n - 1)(to_next.wait_send)
    pl.when(me > 0)(to_prev.wait_send)
    for cond, copy in pending:
        if cond is None:
            copy.wait_send()
        else:
            pl.when(cond)(copy.wait_send)


def local(
    n, features, hint, conv_weight, conv_bias, zero_weight, zero_bias, group_gain, proj_in,
    norm_gain, query_weight, key_weight, value_weight, attn_out, proj_out,
):
    tokens, channels = features.shape
    chips = n // CORES
    rows_a = math.gcd(chips, 4)
    rows_b = chips // rows_a
    sends = 2 + rows_b + (rows_a - 1) * 2 * (1 + rows_b) + (2 * rows_a - 1) * (rows_b - 1)
    square = pltpu.VMEM((channels, channels), BF16)
    vmem = pl.BlockSpec(memory_space=pltpu.VMEM)
    hbm = pl.BlockSpec(memory_space=pl.ANY)
    row = lambda v: v.reshape(1, channels)
    return pl.pallas_call(
        functools.partial(block_kernel, n, rows_a, rows_b),
        out_shape=jax.ShapeDtypeStruct((tokens, channels), BF16),
        in_specs=[vmem] * 6 + [hbm] * 8,
        out_specs=vmem,
        scratch_shapes=[
            pltpu.VMEM(conv_weight.shape, BF16), square, square, square, square, square, square, square,
            pltpu.VMEM((tokens + 2 * WIDTH, channels), BF16),
            pltpu.VMEM((n, tokens, channels), BF16),
            pltpu.VMEM((n * tokens, channels), BF16),
            pltpu.VMEM((channels, HEADS * tokens), BF16),
            pltpu.VMEM((n * tokens, 2 * tokens), F32),
            pltpu.VMEM((channels, tokens), F32),
            pltpu.SemaphoreType.DMA((8,)),
            pltpu.SemaphoreType.DMA((2,)),
            pltpu.SemaphoreType.DMA((2,)),
            pltpu.SemaphoreType.DMA((sends,)),
            pltpu.SemaphoreType.DMA((n,)),
        ],
        compiler_params=pltpu.CompilerParams(
            collective_id=0, has_side_effects=True, vmem_limit_bytes=60 * 1024 * 1024),
    )(features, hint, row(conv_bias), row(zero_bias), row(group_gain), row(norm_gain),
      conv_weight, zero_weight, proj_in, query_weight, key_weight, value_weight, attn_out, proj_out)


def solution(mesh):
    split = P(("dp", "seq"), None)
    return jax.shard_map(
        functools.partial(local, mesh.shape["seq"]), mesh=mesh,
        in_specs=(split, split) + (P(),) * 12, out_specs=split, check_vma=False,
    )
```

```python
import functools
import math

import jax
import jax.numpy as jnp
from jax import lax
from jax.experimental import pallas as pl
from jax.experimental.pallas import tpu as pltpu
from jax.sharding import PartitionSpec as P

HEADS = 8
GROUPS = 32
WIDTH = 128
CORES = 2

norm_eps = 1e-06
layer_eps = 1e-05
MESH = pl.DeviceIdType.MESH
F32 = jnp.float32
BF16 = jnp.bfloat16


def mm(x, y):
    return jnp.dot(x, y, preferred_element_type=F32)


def block_kernel(
    n, rows_a, rows_b,
    features, hint, conv_bias, zero_bias, group_gain, norm_gain,
    conv_hbm, zero_hbm, proj_in_hbm, query_hbm, key_hbm, value_hbm, attn_hbm, proj_hbm,
    out,
    conv_w, zero_w, proj_in_w, query_w, key_w, value_w, attn_w, proj_w,
    ext, gathered, keys_all, keys_t, qmask, scores, mixed,
    load_sem, halo_send, halo_recv, send_sem, recv_sem,
):
    channels, tokens = features.shape
    head_dim = channels // HEADS
    per_group = channels // GROUPS
    me = lax.axis_index("seq")
    core = lax.rem(me, CORES)
    chip = lax.div(me, CORES)
    b = lax.rem(chip, rows_b)
    a = lax.div(chip, rows_b)

    def device(aa, bb, cc):
        return (aa * rows_b + bb) * CORES + cc

    def as_columns(vector):
        return jnp.transpose(jnp.broadcast_to(vector[...].reshape(1, channels), (WIDTH, channels)))[:, :1]

    loads = {}
    for slot, (name, src, dst) in enumerate((
        ("conv", conv_hbm, conv_w), ("zero", zero_hbm, zero_w), ("proj_in", proj_in_hbm, proj_in_w),
        ("query", query_hbm, query_w), ("key", key_hbm, key_w), ("value", value_hbm, value_w),
        ("attn", attn_hbm, attn_w), ("proj", proj_hbm, proj_w),
    )):
        loads[name] = pltpu.make_async_copy(src, dst, load_sem.at[slot])
        loads[name].start()

    barrier = pltpu.get_barrier_semaphore()
    always = jnp.int32(1)
    peers = [
        (me > 0, me - 1), (me < n - 1, me + 1),
        (a > 0, device(a - 1, b, core)), (a < rows_a - 1, device(a + 1, b, core)),
        (None, device(a, b, 1 - core)),
    ]
    for k in range(1, rows_b):
        peers.append((None, device(a, lax.rem(b + k, rows_b), core)))
    count = jnp.int32(0)
    for cond, peer in peers:
        def greet(peer=peer):
            pl.semaphore_signal(barrier, inc=1, device_id={"seq": peer}, device_id_type=MESH)
        if cond is None:
            greet()
            count = count + always
        else:
            pl.when(cond)(greet)
            count = count + cond.astype(jnp.int32)
    pl.semaphore_wait(barrier, count)

    to_next = pltpu.make_async_remote_copy(
        hint.at[:, pl.ds(tokens - WIDTH, WIDTH)], ext.at[:, pl.ds(0, WIDTH)],
        halo_send.at[0], halo_recv.at[0], device_id={"seq": me + 1}, device_id_type=MESH)
    to_prev = pltpu.make_async_remote_copy(
        hint.at[:, pl.ds(0, WIDTH)], ext.at[:, pl.ds(WIDTH + tokens, WIDTH)],
        halo_send.at[1], halo_recv.at[1], device_id={"seq": me - 1}, device_id_type=MESH)
    pl.when(me < n - 1)(to_next.start)
    pl.when(me > 0)(to_prev.start)

    ext[:, pl.ds(WIDTH, tokens)] = hint[...]

    @pl.when(me == 0)
    def _():
        ext[:, pl.ds(0, WIDTH)] = jnp.zeros((channels, WIDTH), BF16)

    @pl.when(me == n - 1)
    def _():
        ext[:, pl.ds(WIDTH + tokens, WIDTH)] = jnp.zeros((channels, WIDTH), BF16)

    middle = jnp.transpose(hint[...])
    loads["conv"].wait()
    taps = [mm(middle, conv_w[1, d]) for d in range(3)]
    pl.when(me > 0)(to_next.wait_recv)
    pl.when(me < n - 1)(to_prev.wait_recv)
    for dy in (0, 2):
        lines = jnp.transpose(ext[:, pl.ds(dy * WIDTH, tokens)])
        taps = [taps[d] + mm(lines, conv_w[dy, d]) for d in range(3)]
    column = lax.rem(lax.broadcasted_iota(jnp.int32, (tokens, channels), 0), WIDTH)
    left = jnp.where(column == 0, 0.0, pltpu.roll(taps[0], 1, 0))
    right = jnp.where(column == WIDTH - 1, 0.0, pltpu.roll(taps[2], tokens - 1, 0))
    conv = left + taps[1] + right + conv_bias[...].reshape(1, channels)
    control = (conv / (1.0 + jnp.exp(-conv))).astype(BF16)
    loads["zero"].wait()
    branch = mm(control, zero_w[...]) + zero_bias[...].reshape(1, channels)
    merged = (features[...].astype(F32) + jnp.transpose(branch)).astype(BF16)
    gathered[me] = merged

    pending = []

    def send(src, target, cond):
        slot = len(pending)
        copy = pltpu.make_async_remote_copy(
            gathered.at[src], gathered.at[src], send_sem.at[slot], recv_sem.at[src],
            device_id={"seq": target}, device_id_type=MESH)
        pending.append((cond, copy))
        if cond is None:
            copy.start()
        else:
            pl.when(cond)(copy.start)

    def arrive(src, cond):
        def wait():
            pltpu.make_async_remote_copy(
                gathered.at[src], gathered.at[src], send_sem.at[0], recv_sem.at[src],
                device_id={"seq": me}, device_id_type=MESH).wait_recv()
        if cond is None:
            wait()
        else:
            pl.when(cond)(wait)

    def both(first, second):
        return second if first is None else first & second

    def to_partner(src, cond):
        send(src, device(a, b, 1 - core), cond)

    def along_b(src, cond):
        for k in range(1, rows_b):
            send(src, device(a, lax.rem(b + k, rows_b), core), cond)

    def from_b(aa, cond):
        for k in range(1, rows_b):
            src = device(aa, lax.rem(b + k, rows_b), core)
            arrive(src, cond)
            yield src

    even, odd = core == 0, core == 1
    up, down = a < rows_a - 1, a > 0

    along_b(me, None)
    send(me, device(a + 1, b, core), up)
    send(me, device(a - 1, b, core), down)
    to_partner(me, None)

    for name in ("proj_in", "query", "key", "value", "attn", "proj"):
        loads[name].wait()
    for weight in (proj_in_w, query_w, value_w, attn_w, proj_w):
        weight[...] = jnp.transpose(weight[...])
    gain, layer_gain = as_columns(group_gain), as_columns(norm_gain)
    row_group = lax.div(lax.broadcasted_iota(jnp.int32, (channels, channels), 0), jnp.int32(per_group))
    col_group = lax.div(lax.broadcasted_iota(jnp.int32, (channels, channels), 1), jnp.int32(per_group))
    same = (row_group == col_group).astype(F32)

    def group_sum(partial):
        total = jnp.dot(same, partial, preferred_element_type=F32, precision=lax.Precision.HIGHEST)
        return jnp.sum(total, axis=1, keepdims=True)

    shift = group_sum(merged.astype(F32)) / (tokens * per_group)

    for src in from_b(a, None):
        send(src, device(a + 1, b, core), even & up)
        send(src, device(a - 1, b, core), even & down)
        to_partner(src, None)
    for step in range(1, rows_a):
        for sign, more in ((-1, up), (1, down)):
            aa = a + sign * step
            inside = (aa >= 0) & (aa < rows_a)
            src = device(aa, b, core)
            arrive(src, inside)
            send(src, device(a - sign, b, core), inside & more)
            along_b(src, inside & odd)
            to_partner(src, inside)
            for k in range(1, rows_b):
                src = device(aa, lax.rem(b + k, rows_b), core)
                arrive(src, inside & even)
                send(src, device(a - sign, b, core), inside & more & even)
                to_partner(src, inside & even)
        for sign in (-1, 1):
            aa = a + sign * step
            inside = (aa >= 0) & (aa < rows_a) & odd
            for src in from_b(aa, inside):
                to_partner(src, inside)

    def add_block(src, acc):
        apart = gathered[src].astype(F32) - shift
        return acc[0] + apart, acc[1] + apart * apart

    zero_acc = jnp.zeros((channels, tokens), F32)
    sums = lax.fori_loop(0, n // CORES, lambda k, acc: add_block(k * CORES + core, acc), (zero_acc, zero_acc))
    for k in range(n // CORES):
        arrive(k * CORES + 1 - core, None)
        sums = add_block(k * CORES + 1 - core, sums)
    entry_count = tokens * n * per_group
    apart_mean = group_sum(sums[0]) / entry_count
    mean = shift + apart_mean
    var = jnp.maximum(group_sum(sums[1]) / entry_count - apart_mean * apart_mean, 0.0)
    inv = lax.rsqrt(var + norm_eps) * gain

    def project_norm(block):
        grouped = ((block.astype(F32) - mean) * inv).astype(BF16)
        inner = mm(proj_in_w[...], grouped).astype(BF16).astype(F32)
        centred = inner - jnp.mean(inner, axis=0, keepdims=True)
        spread = jnp.mean(jnp.square(centred), axis=0, keepdims=True)
        return inner, (centred * lax.rsqrt(spread + layer_eps) * layer_gain).astype(BF16)

    inner_own, normed_own = project_norm(merged)
    chunk = 4 if n % 4 == 0 else 1

    def norm_chunk(k, carry):
        block = jnp.concatenate([gathered[k * chunk + i] for i in range(chunk)], axis=1)
        normed = project_norm(block)[1]
        start = pl.multiple_of(k * chunk * tokens, chunk * tokens)
        keys_t[:, pl.ds(start, chunk * tokens)] = normed
        keys_all[pl.ds(start, chunk * tokens)] = jnp.transpose(normed)
        return carry

    lax.fori_loop(0, n // chunk, norm_chunk, 0)

    queries = mm(query_w[...], normed_own)
    row_head = lax.div(lax.broadcasted_iota(jnp.int32, (channels, tokens), 0), jnp.int32(head_dim))
    for h in range(HEADS):
        qmask[:, h * tokens:(h + 1) * tokens] = jnp.where(row_head == h, queries, 0.0).astype(BF16)
    scale = math.log2(math.e) / math.sqrt(head_dim)
    qmask[...] = (mm(key_w[...], qmask[...]) * scale).astype(BF16)

    pair = 2 * tokens
    for h2 in range(HEADS // 2):
        cols = slice(h2 * pair, (h2 + 1) * pair)
        scores[...] = mm(keys_all[...], qmask[:, cols])
        top = jnp.max(scores[...], axis=0, keepdims=True)
        weights = jnp.exp2(scores[...] - top)
        total = jnp.sum(weights, axis=0, keepdims=True)
        folded = (mm(keys_t[...], weights.astype(BF16)) / total).astype(BF16)
        values = mm(value_w[...], folded)
        for j in range(2):
            h = 2 * h2 + j
            mixed[pl.ds(h * head_dim, head_dim)] = values[h * head_dim:(h + 1) * head_dim, j * tokens:(j + 1) * tokens]
    after = (inner_own + mm(attn_w[...], mixed[...].astype(BF16))).astype(BF16)
    out[...] = (merged.astype(F32) + mm(proj_w[...], after)).astype(BF16)

    pl.when(me < n - 1)(to_next.wait_send)
    pl.when(me > 0)(to_prev.wait_send)
    for cond, copy in pending:
        if cond is None:
            copy.wait_send()
        else:
            pl.when(cond)(copy.wait_send)


def local(
    n, features, hint, conv_weight, conv_bias, zero_weight, zero_bias, group_gain, proj_in,
    norm_gain, query_weight, key_weight, value_weight, attn_out, proj_out,
):
    tokens, channels = features.shape
    chips = n // CORES
    rows_a = math.gcd(chips, 4)
    rows_b = chips // rows_a
    sends = 2 + rows_b + 3 * (rows_b - 1) + (rows_a - 1) * 2 * (1 + rows_b + 3 * (rows_b - 1))
    square = pltpu.VMEM((channels, channels), BF16)
    vmem = pl.BlockSpec(memory_space=pltpu.VMEM)
    hbm = pl.BlockSpec(memory_space=pl.ANY)
    result = pl.pallas_call(
        functools.partial(block_kernel, n, rows_a, rows_b),
        out_shape=jax.ShapeDtypeStruct((channels, tokens), BF16),
        in_specs=[vmem] * 6 + [hbm] * 8,
        out_specs=vmem,
        scratch_shapes=[
            pltpu.VMEM(conv_weight.shape, BF16), square, square, square, square, square, square, square,
            pltpu.VMEM((channels, tokens + 2 * WIDTH), BF16),
            pltpu.VMEM((n, channels, tokens), BF16),
            pltpu.VMEM((n * tokens, channels), BF16),
            pltpu.VMEM((channels, n * tokens), BF16),
            pltpu.VMEM((channels, HEADS * tokens), BF16),
            pltpu.VMEM((n * tokens, 2 * tokens), F32),
            pltpu.VMEM((channels, tokens), F32),
            pltpu.SemaphoreType.DMA((8,)),
            pltpu.SemaphoreType.DMA((2,)),
            pltpu.SemaphoreType.DMA((2,)),
            pltpu.SemaphoreType.DMA((sends,)),
            pltpu.SemaphoreType.DMA((n,)),
        ],
        compiler_params=pltpu.CompilerParams(
            collective_id=0, has_side_effects=True, vmem_limit_bytes=60 * 1024 * 1024),
    )(features.T, hint.T, conv_bias, zero_bias, group_gain, norm_gain,
      conv_weight, zero_weight, proj_in, query_weight, key_weight, value_weight, attn_out, proj_out)
    return result.T


def solution(mesh):
    split = P(("dp", "seq"), None)
    return jax.shard_map(
        functools.partial(local, mesh.shape["seq"]), mesh=mesh,
        in_specs=(split, split) + (P(),) * 12, out_specs=split, check_vma=False,
    )
```

```python
import functools
import math

import jax
import jax.numpy as jnp
from jax import lax
from jax.experimental import pallas as pl
from jax.experimental.pallas import tpu as pltpu
from jax.sharding import PartitionSpec as P

HEADS = 8
GROUPS = 32
WIDTH = 128
CORES = 2

norm_eps = 1e-06
layer_eps = 1e-05
MESH = pl.DeviceIdType.MESH
F32 = jnp.float32
BF16 = jnp.bfloat16


def mm(x, y):
    return jnp.dot(x, y, preferred_element_type=F32)


def block_kernel(
    n, rows_a, rows_b,
    features, hint, conv_bias, zero_bias, group_gain, norm_gain,
    conv_hbm, zero_hbm, proj_in_hbm, query_hbm, key_hbm, value_hbm, attn_hbm, proj_hbm,
    out,
    conv_w, zero_w, proj_in_w, query_w, key_w, value_w, attn_w, proj_w,
    ext, gathered, keys_all, keys_t, qmask, scores, mixed,
    load_sem, halo_send, halo_recv, send_sem, recv_sem,
):
    channels, tokens = features.shape
    head_dim = channels // HEADS
    per_group = channels // GROUPS
    me = lax.axis_index("seq")
    core = lax.rem(me, CORES)
    chip = lax.div(me, CORES)
    b = lax.rem(chip, rows_b)
    a = lax.div(chip, rows_b)

    def device(aa, bb, cc):
        return (aa * rows_b + bb) * CORES + cc

    def as_columns(vector):
        return jnp.transpose(jnp.broadcast_to(vector[...].reshape(1, channels), (WIDTH, channels)))[:, :1]

    loads = {}
    for slot, (name, src, dst) in enumerate((
        ("conv", conv_hbm, conv_w), ("zero", zero_hbm, zero_w), ("proj_in", proj_in_hbm, proj_in_w),
        ("query", query_hbm, query_w), ("key", key_hbm, key_w), ("value", value_hbm, value_w),
        ("attn", attn_hbm, attn_w), ("proj", proj_hbm, proj_w),
    )):
        loads[name] = pltpu.make_async_copy(src, dst, load_sem.at[slot])
        loads[name].start()

    barrier = pltpu.get_barrier_semaphore()
    always = jnp.int32(1)
    peers = [
        (me > 0, me - 1), (me < n - 1, me + 1),
        (a > 0, device(a - 1, b, core)), (a < rows_a - 1, device(a + 1, b, core)),
        (None, device(a, b, 1 - core)),
    ]
    for k in range(1, rows_b):
        peers.append((None, device(a, lax.rem(b + k, rows_b), core)))
    count = jnp.int32(0)
    for cond, peer in peers:
        def greet(peer=peer):
            pl.semaphore_signal(barrier, inc=1, device_id={"seq": peer}, device_id_type=MESH)
        if cond is None:
            greet()
            count = count + always
        else:
            pl.when(cond)(greet)
            count = count + cond.astype(jnp.int32)
    pl.semaphore_wait(barrier, count)

    to_next = pltpu.make_async_remote_copy(
        hint.at[:, pl.ds(tokens - WIDTH, WIDTH)], ext.at[:, pl.ds(0, WIDTH)],
        halo_send.at[0], halo_recv.at[0], device_id={"seq": me + 1}, device_id_type=MESH)
    to_prev = pltpu.make_async_remote_copy(
        hint.at[:, pl.ds(0, WIDTH)], ext.at[:, pl.ds(WIDTH + tokens, WIDTH)],
        halo_send.at[1], halo_recv.at[1], device_id={"seq": me - 1}, device_id_type=MESH)
    pl.when(me < n - 1)(to_next.start)
    pl.when(me > 0)(to_prev.start)

    ext[:, pl.ds(WIDTH, tokens)] = hint[...]

    @pl.when(me == 0)
    def _():
        ext[:, pl.ds(0, WIDTH)] = jnp.zeros((channels, WIDTH), BF16)

    @pl.when(me == n - 1)
    def _():
        ext[:, pl.ds(WIDTH + tokens, WIDTH)] = jnp.zeros((channels, WIDTH), BF16)

    middle = jnp.transpose(hint[...])
    loads["conv"].wait()
    taps = [mm(middle, conv_w[1, d]) for d in range(3)]
    pl.when(me > 0)(to_next.wait_recv)
    pl.when(me < n - 1)(to_prev.wait_recv)
    for dy in (0, 2):
        lines = jnp.transpose(ext[:, pl.ds(dy * WIDTH, tokens)])
        taps = [taps[d] + mm(lines, conv_w[dy, d]) for d in range(3)]
    column = lax.rem(lax.broadcasted_iota(jnp.int32, (tokens, channels), 0), WIDTH)
    left = jnp.where(column == 0, 0.0, pltpu.roll(taps[0], 1, 0))
    right = jnp.where(column == WIDTH - 1, 0.0, pltpu.roll(taps[2], tokens - 1, 0))
    conv = left + taps[1] + right + conv_bias[...].reshape(1, channels)
    control = (conv / (1.0 + jnp.exp(-conv))).astype(BF16)
    loads["zero"].wait()
    branch = mm(control, zero_w[...]) + zero_bias[...].reshape(1, channels)
    merged = (features[...].astype(F32) + jnp.transpose(branch)).astype(BF16)
    gathered[me] = merged

    pending = []

    def send(src, target, cond):
        slot = len(pending)
        copy = pltpu.make_async_remote_copy(
            gathered.at[src], gathered.at[src], send_sem.at[slot], recv_sem.at[src],
            device_id={"seq": target}, device_id_type=MESH)
        pending.append((cond, copy))
        if cond is None:
            copy.start()
        else:
            pl.when(cond)(copy.start)

    def arrive(src, cond):
        def wait():
            pltpu.make_async_remote_copy(
                gathered.at[src], gathered.at[src], send_sem.at[0], recv_sem.at[src],
                device_id={"seq": me}, device_id_type=MESH).wait_recv()
        if cond is None:
            wait()
        else:
            pl.when(cond)(wait)

    def both(first, second):
        return second if first is None else first & second

    def to_partner(src, cond):
        send(src, device(a, b, 1 - core), cond)

    def along_b(src, cond):
        for k in range(1, rows_b):
            send(src, device(a, lax.rem(b + k, rows_b), core), cond)

    def from_b(aa, cond):
        for k in range(1, rows_b):
            src = device(aa, lax.rem(b + k, rows_b), core)
            arrive(src, cond)
            yield src

    even, odd = core == 0, core == 1
    up, down = a < rows_a - 1, a > 0

    along_b(me, None)
    send(me, device(a + 1, b, core), up)
    send(me, device(a - 1, b, core), down)
    to_partner(me, None)

    for name in ("proj_in", "query", "key", "value", "attn", "proj"):
        loads[name].wait()
    for weight in (proj_in_w, query_w, value_w, attn_w, proj_w):
        weight[...] = jnp.transpose(weight[...])
    gain, layer_gain = as_columns(group_gain), as_columns(norm_gain)
    row_group = lax.div(lax.broadcasted_iota(jnp.int32, (channels, channels), 0), jnp.int32(per_group))
    col_group = lax.div(lax.broadcasted_iota(jnp.int32, (channels, channels), 1), jnp.int32(per_group))
    same = (row_group == col_group).astype(F32)

    def group_sum(partial):
        total = jnp.dot(same, partial, preferred_element_type=F32, precision=lax.Precision.HIGHEST)
        return jnp.sum(total, axis=1, keepdims=True)

    shift = group_sum(merged.astype(F32)) / (tokens * per_group)

    for src in from_b(a, None):
        send(src, device(a + 1, b, core), even & up)
        send(src, device(a - 1, b, core), even & down)
        to_partner(src, None)
    for step in range(1, rows_a):
        for sign, more in ((-1, up), (1, down)):
            aa = a + sign * step
            inside = (aa >= 0) & (aa < rows_a)
            src = device(aa, b, core)
            arrive(src, inside)
            send(src, device(a - sign, b, core), inside & more)
            along_b(src, inside & odd)
            to_partner(src, inside)
            for k in range(1, rows_b):
                src = device(aa, lax.rem(b + k, rows_b), core)
                arrive(src, inside & even)
                send(src, device(a - sign, b, core), inside & more & even)
                to_partner(src, inside & even)
        for sign in (-1, 1):
            aa = a + sign * step
            inside = (aa >= 0) & (aa < rows_a) & odd
            for src in from_b(aa, inside):
                to_partner(src, inside)

    def add_block(src, acc):
        apart = gathered[src].astype(F32) - shift
        return acc[0] + apart, acc[1] + apart * apart

    zero_acc = jnp.zeros((channels, tokens), F32)
    sums = lax.fori_loop(0, n // CORES, lambda k, acc: add_block(k * CORES + core, acc), (zero_acc, zero_acc))
    for k in range(n // CORES):
        arrive(k * CORES + 1 - core, None)
        sums = add_block(k * CORES + 1 - core, sums)
    entry_count = tokens * n * per_group
    apart_mean = group_sum(sums[0]) / entry_count
    mean = shift + apart_mean
    var = jnp.maximum(group_sum(sums[1]) / entry_count - apart_mean * apart_mean, 0.0)
    inv = lax.rsqrt(var + norm_eps) * gain

    def project_norm(block):
        grouped = ((block.astype(F32) - mean) * inv).astype(BF16)
        inner = mm(proj_in_w[...], grouped).astype(BF16).astype(F32)
        centred = inner - jnp.mean(inner, axis=0, keepdims=True)
        spread = jnp.mean(jnp.square(centred), axis=0, keepdims=True)
        return inner, (centred * lax.rsqrt(spread + layer_eps) * layer_gain).astype(BF16)

    inner_own, normed_own = project_norm(merged)
    chunk = 4 if n % 4 == 0 else 1

    def norm_chunk(k, carry):
        block = jnp.concatenate([gathered[k * chunk + i] for i in range(chunk)], axis=1)
        normed = project_norm(block)[1]
        start = pl.multiple_of(k * chunk * tokens, chunk * tokens)
        keys_t[:, pl.ds(start, chunk * tokens)] = normed
        keys_all[pl.ds(start, chunk * tokens)] = jnp.transpose(normed)
        return carry

    lax.fori_loop(0, n // chunk, norm_chunk, 0)

    queries = mm(query_w[...], normed_own)
    row_head = lax.div(lax.broadcasted_iota(jnp.int32, (channels, tokens), 0), jnp.int32(head_dim))
    for h in range(HEADS):
        qmask[:, h * tokens:(h + 1) * tokens] = jnp.where(row_head == h, queries, 0.0).astype(BF16)
    scale = math.log2(math.e) / math.sqrt(head_dim)
    qmask[...] = (mm(key_w[...], qmask[...]) * scale).astype(BF16)

    pair = 2 * tokens
    def score(h2):
        scores[h2 % 2] = mm(keys_all[...], qmask[:, h2 * pair:(h2 + 1) * pair])

    score(0)
    for h2 in range(HEADS // 2):
        if h2 + 1 < HEADS // 2:
            score(h2 + 1)
        top = jnp.max(scores[h2 % 2], axis=0, keepdims=True)
        weights = jnp.exp2(scores[h2 % 2] - top)
        total = jnp.sum(weights, axis=0, keepdims=True)
        folded = (mm(keys_t[...], weights.astype(BF16)) / total).astype(BF16)
        values = mm(value_w[...], folded)
        for j in range(2):
            h = 2 * h2 + j
            mixed[pl.ds(h * head_dim, head_dim)] = values[h * head_dim:(h + 1) * head_dim, j * tokens:(j + 1) * tokens]
    after = (inner_own + mm(attn_w[...], mixed[...].astype(BF16))).astype(BF16)
    out[...] = (merged.astype(F32) + mm(proj_w[...], after)).astype(BF16)

    pl.when(me < n - 1)(to_next.wait_send)
    pl.when(me > 0)(to_prev.wait_send)
    for cond, copy in pending:
        if cond is None:
            copy.wait_send()
        else:
            pl.when(cond)(copy.wait_send)


def local(
    n, features, hint, conv_weight, conv_bias, zero_weight, zero_bias, group_gain, proj_in,
    norm_gain, query_weight, key_weight, value_weight, attn_out, proj_out,
):
    tokens, channels = features.shape
    chips = n // CORES
    rows_a = math.gcd(chips, 4)
    rows_b = chips // rows_a
    sends = 2 + rows_b + 3 * (rows_b - 1) + (rows_a - 1) * 2 * (1 + rows_b + 3 * (rows_b - 1))
    square = pltpu.VMEM((channels, channels), BF16)
    vmem = pl.BlockSpec(memory_space=pltpu.VMEM)
    hbm = pl.BlockSpec(memory_space=pl.ANY)
    result = pl.pallas_call(
        functools.partial(block_kernel, n, rows_a, rows_b),
        out_shape=jax.ShapeDtypeStruct((channels, tokens), BF16),
        in_specs=[vmem] * 6 + [hbm] * 8,
        out_specs=vmem,
        scratch_shapes=[
            pltpu.VMEM(conv_weight.shape, BF16), square, square, square, square, square, square, square,
            pltpu.VMEM((channels, tokens + 2 * WIDTH), BF16),
            pltpu.VMEM((n, channels, tokens), BF16),
            pltpu.VMEM((n * tokens, channels), BF16),
            pltpu.VMEM((channels, n * tokens), BF16),
            pltpu.VMEM((channels, HEADS * tokens), BF16),
            pltpu.VMEM((2, n * tokens, 2 * tokens), F32),
            pltpu.VMEM((channels, tokens), F32),
            pltpu.SemaphoreType.DMA((8,)),
            pltpu.SemaphoreType.DMA((2,)),
            pltpu.SemaphoreType.DMA((2,)),
            pltpu.SemaphoreType.DMA((sends,)),
            pltpu.SemaphoreType.DMA((n,)),
        ],
        compiler_params=pltpu.CompilerParams(
            collective_id=0, has_side_effects=True, vmem_limit_bytes=60 * 1024 * 1024),
    )(features.T, hint.T, conv_bias, zero_bias, group_gain, norm_gain,
      conv_weight, zero_weight, proj_in, query_weight, key_weight, value_weight, attn_out, proj_out)
    return result.T


def solution(mesh):
    split = P(("dp", "seq"), None)
    return jax.shard_map(
        functools.partial(local, mesh.shape["seq"]), mesh=mesh,
        in_specs=(split, split) + (P(),) * 12, out_specs=split, check_vma=False,
    )
```
